32 devices in a mesh: gx: 4 (over y, core), gy: 8 (over z, x).
Axes of the slice: x: 2, y: 2, z: 4, core: 2. Of those that a mesh axis runs over, the one named last changes fastest.
Arguments:
- right_side: float32 [128, 256, 512], P('gx', 'gy'), as said below
- start_guess: float32 [128, 256, 512], P('gx', 'gy'), may hold values from -3 to 3
- conductivity: float32 [128, 256, 512], P('gx', 'gy'), may hold values from 0.5 to 8
Outputs:
- solution_field: float32 [128, 256, 512], P('gx', 'gy')
- estimate: float32 [], replicated
The draws below stay inside these ranges and needn't reach their ends.
Inputs may be any that keep to these rules, and one draw needn't show every extreme that they name: `right_side`: A smoothly varying positive scale times noise, which may have a nonzero mean.
All inputs are finite; a program needn't handle non-finite values.
Results may differ from the reference program's by a relative error of at most 0.0003.
Values sent between devices are 32-bit elements; how exact they have to be, the bound alone decides.
No kernel may reach another device: no remote copies, remote signals or barrier semaphores. Data moves between devices by JAX's collectives and lax.ppermute only.
A program may use at most 64 MiB of HBM per device.

```python
import math
import jax
import jax.numpy as jnp
from jax import lax

CZ = 512
M = 3
NX = 128
NY = 256


def draw_right_side(key, part):
    noise = jax.random.normal(jax.random.fold_in(key, 7), (NX, NY, CZ), jnp.float32)
    first = (jnp.arange(NX, dtype=jnp.float32) / NX)[:, None, None]
    second = (jnp.arange(NY, dtype=jnp.float32) / NY)[None, :, None]
    scale = (0.5 + first) * (0.5 + second)
    return scale * noise


def block_levels(rng, shape, split, least, high):
    loudness, own = 1.0, jax.random.fold_in(rng, 6)
    for axis_at, blocks in split:
        steps = jnp.exp(jax.random.uniform(jax.random.fold_in(own, axis_at), (blocks,), jnp.float32, least / len(split), high / len(split)))
        loudness = loudness * jnp.repeat(steps, shape[axis_at] // blocks).reshape([-1 if axis == axis_at else 1 for axis in range(len(shape))])
    return loudness


def normal_values(rng, shape, deviation, bound, split=(), kind=jnp.bfloat16):
    drawn = jax.random.normal(rng, shape, jnp.float32) * deviation
    if len(split) > 0:
        drawn = block_levels(rng, shape, split, -0.22, 0.18) * drawn
    return jnp.clip(drawn, min=-bound, max=bound).astype(kind)


def setup_inputs(seed: int = 0) -> dict:
    keys = jax.random.split(jax.random.key(seed), 4)
    return {
        "right_side": draw_right_side(jax.random.fold_in(keys[3], 71), 0),
        "start_guess": normal_values(keys[1], (NX, NY, CZ), 0.5, 3.0, ((0, 4), (1, 8)), jnp.float32),
        "conductivity": jnp.clip(jnp.exp(math.log(8.0) - 2.7725887 * jax.random.uniform(keys[2], (NX, NY, CZ), jnp.float32) ** block_levels(keys[2], (NX, NY, CZ), ((0, 4), (1, 8)), -0.2, 0.2)), 0.5, 8.0),
    }


def shifted(padded, which, sign):
    starts = [1, 1, 1]
    starts[which] = 1 + sign
    limits = [starts[dim] + padded.shape[dim] - 2 for dim in range(3)]
    return lax.slice(padded, starts, limits)

def stencil(padded, kappa_pad):
    centre = shifted(padded, 0, 0)
    middle = shifted(kappa_pad, 0, 0)
    result = jnp.zeros_like(centre)
    for which in range(3):
        for sign in (-1, 1):
            result = result + 0.5 * (middle + shifted(kappa_pad, which, sign)) * (centre - shifted(padded, which, sign))
    return result

def least_squares(columns, beta):
    count = len(columns)
    rhs_vals = [beta] + [jnp.float32(0.0)] * count
    cosines = []
    sines = []
    upper = []
    for column in range(count):
        entries = list(columns[column])
        for earlier in range(column):
            first = entries[earlier]
            second = entries[earlier + 1]
            entries[earlier] = cosines[earlier] * first + sines[earlier] * second
            entries[earlier + 1] = -sines[earlier] * first + cosines[earlier] * second
        first = entries[column]
        second = entries[column + 1]
        radius = jnp.sqrt(first * first + second * second)
        cosines.append(first / radius)
        sines.append(second / radius)
        entries[column] = radius
        rhs_vals[column + 1] = -sines[column] * rhs_vals[column]
        rhs_vals[column] = cosines[column] * rhs_vals[column]
        upper.append(entries[:column + 1])
    coeffs = [None] * count
    for row in reversed(range(count)):
        value = rhs_vals[row]
        for later in range(row + 1, count):
            value = value - upper[later][row] * coeffs[later]
        coeffs[row] = value / upper[row][row]
    return (coeffs, jnp.abs(rhs_vals[count]))

def reference(right_side, start_guess, conductivity):
    kappa_pad = jnp.pad(conductivity, 1)
    start = right_side - stencil(jnp.pad(start_guess, 1), kappa_pad)
    beta = jnp.sqrt(jnp.sum(start * start))
    basis = [start / beta]
    columns = []
    for column in range(M):
        vector = stencil(jnp.pad(basis[column], 1), kappa_pad)
        entries = []
        for earlier in range(column + 1):
            coeff = jnp.sum(vector * basis[earlier])
            vector = vector - coeff * basis[earlier]
            entries.append(coeff)
        length = jnp.sqrt(jnp.sum(vector * vector))
        entries.append(length)
        columns.append(entries)
        basis.append(vector / length)
    coeffs, estimate = least_squares(columns, beta)
    solution_field = start_guess
    for column in range(M):
        solution_field = solution_field + coeffs[column] * basis[column]
    return (solution_field, estimate)
```

```python
import functools

import jax
import jax.numpy as jnp
from jax import lax
from jax.experimental import pallas as pl
from jax.experimental.pallas import tpu as pltpu
from jax.sharding import PartitionSpec as P

M = 3
SCALE = 128.0
SMALL = 2.0**-14
VMEM_SPEC = pl.BlockSpec(memory_space=pltpu.VMEM)
ANY_SPEC = pl.BlockSpec(memory_space=pl.ANY)
F32 = jnp.float32


def vmem(shape):
    return pltpu.VMEM(shape, F32)


def call(body, out_shape, n_in, flops=0, scratch=(), aliases=None, any_in=(), any_out=(), name=None):
    outs = list(out_shape)
    return pl.pallas_call(
        body,
        out_shape=outs,
        in_specs=[ANY_SPEC if i in any_in else VMEM_SPEC for i in range(n_in)],
        out_specs=[ANY_SPEC if i in any_out else VMEM_SPEC for i in range(len(outs))],
        scratch_shapes=list(scratch),
        input_output_aliases=aliases or {},
        cost_estimate=pl.CostEstimate(flops=flops, bytes_accessed=0, transcendentals=0),
        compiler_params=pltpu.CompilerParams(vmem_limit_bytes=16 * 1024 * 1024),
        name=name,
    )


def pairings(sizes):
    nx, ny = sizes
    at = lambda i, j: i * ny + j
    ends = lambda i, n: i == 0 or i == n - 1
    gx_a, gx_b, gy_a, gy_b = [], [], [], []
    for i in range(nx):
        for j in range(ny):
            gx_a.append((at(i, j), at(i ^ 1, j)))
            gy_a.append((at(i, j), at(i, j ^ 1)))
            gx_b.append((at(i, j), at(nx - 1 - i if ends(i, nx) else ((i + 1) ^ 1) - 1, j)))
            gy_b.append((at(i, j), at(i ^ 1, j) if ends(j, ny) else at(i, ((j + 1) ^ 1) - 1)))
    return gx_a, gx_b, gy_a, gy_b


def exchange(parts, sizes):
    moved = [lax.ppermute(part, ("gx", "gy"), pairs) for part, pairs in zip(parts, pairings(sizes))]
    return moved


def sides(sizes, shape):
    out = []
    for name, count, rows in (("gx", sizes[0], shape[0]), ("gy", sizes[1], shape[1])):
        index = lax.axis_index(name)
        odd = lax.rem(index, 2)
        inside = jnp.logical_and(index > 0, index < count - 1)
        out.append(((1 - odd) * (rows - 1), odd * (rows - 1), inside))
    return out


def faces_kernel(sizes, x_hbm, k_hbm, x_ref, k_ref, xa, xb, ya, yb, sem):
    copies = [pltpu.make_async_copy(k_hbm, k_ref, sem.at[0]), pltpu.make_async_copy(x_hbm, x_ref, sem.at[1])]
    for copy in copies:
        copy.start()
    (ax, bx, _), (ay, by, _) = sides(sizes, x_ref.shape)
    for copy in copies:
        copy.wait()
    for at, ref in enumerate((x_ref, k_ref)):
        xa[at] = ref[ax]
        xb[at] = ref[bx]
        for row in range(ref.shape[0]):
            ya[at, pl.ds(row, 1)] = ref[row, pl.ds(ay, 1)]
            yb[at, pl.ds(row, 1)] = ref[row, pl.ds(by, 1)]


def tree(parts):
    while len(parts) > 1:
        parts = [parts[i] + parts[i + 1] if i + 1 < len(parts) else parts[i] for i in range(0, len(parts), 2)]
    return parts[0]


def folded(plane):
    rows, lanes = plane.shape
    return tree([plane[r : r + 8, c : c + 128] for r in range(0, rows, 8) for c in range(0, lanes, 128)])


def applied(u_ref, x, cx_lo, cx_hi, cy, cz, end):
    last = u_ref.shape[0] - 1
    rows, lanes = u_ref.shape[1:]
    u = u_ref[x]
    w = cx_hi * (u - u_ref[jnp.minimum(x + 1, last)]) + cx_lo * (u - u_ref[jnp.maximum(x - 1, 0)])
    flux = cy * (u - pltpu.roll(u, rows - 1, 0))
    w = w + (flux - pltpu.roll(flux, 1, 0))
    flux = cz * (u - pltpu.roll(u, lanes - 1, 1))
    return u, w + (flux - pltpu.roll(flux, 1, 1)) + end * u


def start_kernel(x_ref, k_ref, b_hbm, r_ref, cx_ref, cy_ref, cz_ref, end_ref, b_ref, sem):
    planes, rows, lanes = x_ref.shape
    step = 8
    copies = [
        pltpu.make_async_copy(b_hbm.at[pl.ds(p, step)], b_ref.at[pl.ds(p, step)], sem.at[p // step])
        for p in range(0, planes, step)
    ]
    for copy in copies:
        copy.start()
    row = lax.broadcasted_iota(jnp.int32, (rows, lanes), 0)
    lane = lax.broadcasted_iota(jnp.int32, (rows, lanes), 1)
    half = 0.5 / SCALE
    cx_ref[0] = jnp.zeros((rows, lanes), F32)

    def plane(x, carry):
        k = k_ref[x]
        above = k_ref[jnp.minimum(x + 1, planes - 1)]
        cx_hi = jnp.where(x == planes - 1, 0.0, half * (k + above))
        cy = jnp.where(row == rows - 1, 0.0, half * (k + pltpu.roll(k, rows - 1, 0)))
        cz = jnp.where(lane == lanes - 1, 0.0, half * (k + pltpu.roll(k, lanes - 1, 1)))
        end = jnp.where(jnp.logical_or(lane == 0, lane == lanes - 1), half * k, 0.0)
        cx_ref[x + 1] = cx_hi
        cy_ref[x] = cy
        cz_ref[x] = cz
        end_ref[x] = end
        _, w = applied(x_ref, x, cx_ref[x], cx_hi, cy, cz, end)
        r_ref[x] = b_ref[x] - SCALE * w
        return carry

    for at, copy in enumerate(copies):
        copy.wait()
        lax.fori_loop(at * step, (at + 1) * step, plane, 0)


def apply_kernel(with_older, last, *refs):
    u_ref, cx_ref, cy_ref, cz_ref, end_ref = refs[:5]
    older_ref = refs[5] if with_older else None
    w_ref, dots_ref = refs[-2:]
    planes = u_ref.shape[0]

    def plane(x, sums):
        u, w = applied(u_ref, x, cx_ref[x], cx_ref[x + 1], cy_ref[x], cz_ref[x], end_ref[x])
        w_ref[x] = w
        terms = [u * u]
        if with_older:
            terms.append(u * older_ref[x])
        if last:
            terms += [u * w, w * w]
        return tuple(s + folded(t) for s, t in zip(sums, terms))

    count = 1 + with_older + 2 * last
    sums = lax.fori_loop(0, planes, plane, tuple(jnp.zeros((8, 128), F32) for _ in range(count)))
    for at, s in enumerate(sums):
        dots_ref[at] = s


def start_fix_kernel(sizes, r_in, sxa, sxb, sya, syb, hxa, hxb, hya, hyb, r_ref, cxa, cxb, cya, cyb, oxa, oxb, oya, oyb):
    (ax, bx, in_x), (ay, by, in_y) = sides(sizes, r_ref.shape)
    half = 0.5 / SCALE

    def terms(sent, halo, inside):
        field, k = halo[0], halo[1]
        if inside is not None:
            field, k = jnp.where(inside, field, 0.0), jnp.where(inside, k, 0.0)
        c = half * (sent[1] + k)
        return c, SCALE * (c * (sent[0] - field))

    cxa[...], dxa = terms(sxa, hxa, None)
    cxb[...], dxb = terms(sxb, hxb, in_x)
    cya[...], dya = terms(sya, hya, None)
    cyb[...], dyb = terms(syb, hyb, in_y)
    r_ref[ax] = r_ref[ax] - dxa
    r_ref[bx] = r_ref[bx] - dxb
    for row in range(r_ref.shape[0]):
        for at, d, out in ((ay, dya, oya), (by, dyb, oyb)):
            new = r_ref[row, pl.ds(at, 1)] - d[row : row + 1]
            r_ref[row, pl.ds(at, 1)] = new
            out[pl.ds(row, 1)] = new
    oxa[...] = r_ref[ax]
    oxb[...] = r_ref[bx]


def fix_terms(sizes, shape, sends, halos, coeffs):
    (ax, bx, in_x), (ay, by, in_y) = sides(sizes, shape)
    out = []
    for sent, halo, c, inside in zip(sends, halos, coeffs, (None, in_x, None, in_y)):
        field = halo[...]
        if inside is not None:
            field = jnp.where(inside, field, 0.0)
        out.append(c[...] * (sent[...] - field))
    return (ax, bx, ay, by), out


def fix_kernel(sizes, w_in, *refs):
    sends, halos, coeffs, (w_ref, oxa, oxb, oya, oyb) = refs[:4], refs[4:8], refs[8:12], refs[12:]
    (ax, bx, ay, by), (dxa, dxb, dya, dyb) = fix_terms(sizes, w_ref.shape, sends, halos, coeffs)
    w_ref[ax] = w_ref[ax] + dxa
    w_ref[bx] = w_ref[bx] + dxb
    for row in range(w_ref.shape[0]):
        for at, d, out in ((ay, dya, oya), (by, dyb, oyb)):
            new = w_ref[row, pl.ds(at, 1)] + d[row : row + 1]
            w_ref[row, pl.ds(at, 1)] = new
            out[pl.ds(row, 1)] = new
    oxa[...] = w_ref[ax]
    oxb[...] = w_ref[bx]


def two_sum(a, b):
    s = a + b
    t = s - a
    return s, (a - (s - t)) + (b - t)


def split(a):
    t = 4097.0 * a
    high = t - (t - a)
    return high, a - high


def two_product(a, b):
    p = a * b
    ah, al = split(a)
    bh, bl = split(b)
    return p, ((ah * bh - p) + ah * bl + al * bh) + al * bl


def minus_product(value, factor, other):
    p, e = two_product(factor, other[0])
    s, t = two_sum(value[0], -p)
    t = t + ((value[1] - e) - factor * other[1])
    high = s + t
    return high, t - (high - s)


def folds(high, low, axis):
    shift = high.shape[axis] // 2
    while shift:
        high, err = two_sum(high, pltpu.roll(high, shift, axis))
        low = low + pltpu.roll(low, shift, axis) + err
        shift //= 2
    return high, low


def last_fix_kernel(sizes, w_in, *refs):
    sends, halos, coeffs = refs[:4], refs[4:8], refs[8:12]
    dots0, dots1, dots2, w_ref, out_ref = refs[12:]
    (ax, bx, ay, by), (dxa, dxb, dya, dyb) = fix_terms(sizes, w_ref.shape, sends, halos, coeffs)
    cross, square = [], []
    for at, d, sent in ((ax, dxa, sends[0]), (bx, dxb, sends[1])):
        old = w_ref[at]
        w_ref[at] = old + d
        cross.append(folded(d * sent[...]))
        square.append(folded(d * (old + old + d)))
    for at, d, sent in ((ay, dya, sends[2]), (by, dyb, sends[3])):
        old = jnp.concatenate([w_ref[row, pl.ds(at, 1)] for row in range(w_ref.shape[0])], axis=0)
        cross.append(folded(d * sent[...]))
        square.append(folded(d * (old + old + d)))
    zero = jnp.zeros((8, 128), F32)
    m5 = two_sum(dots2[2], tree(cross))
    m6 = two_sum(dots2[3], tree(square))
    moments = [(dots0[0], zero), (dots1[1], zero), (dots1[0], zero), (dots2[1], zero), (dots2[0], zero), m5, m6]
    sub = lax.broadcasted_iota(jnp.int32, (8, 128), 0)
    lane = lax.broadcasted_iota(jnp.int32, (8, 128), 1)
    high, low = zero, zero
    for at, (h, l) in enumerate(moments):
        h, l = folds(h, l, 0)
        high = jnp.where(sub == at, h, high)
        low = jnp.where(sub == at, l, low)
    high, low = folds(high, low, 1)
    flat = jnp.where(lane == sub, high, jnp.where(lane == sub + 8, low, 0.0))
    for shift in (4, 2, 1):
        flat = flat + pltpu.roll(flat, shift, 0)
    for at in range(out_ref.shape[0]):
        out_ref[at] = flat[0:1]


def least_squares(alphas, offs):
    one = jnp.ones_like(alphas[0])
    rhs = [one] + [jnp.zeros_like(one)] * M
    cosines, sines, upper = [], [], []
    for column in range(M):
        entries = [jnp.zeros_like(one)] * (column + 2)
        if column:
            entries[column - 1] = offs[column - 1]
        entries[column] = alphas[column]
        entries[column + 1] = offs[column]
        for earlier in range(column):
            first, second = entries[earlier], entries[earlier + 1]
            entries[earlier] = cosines[earlier] * first + sines[earlier] * second
            entries[earlier + 1] = cosines[earlier] * second - sines[earlier] * first
        first, second = entries[column], entries[column + 1]
        radius = jnp.sqrt(first * first + second * second)
        cosines.append(first / radius)
        sines.append(second / radius)
        entries[column] = radius
        rhs[column + 1] = -sines[column] * rhs[column]
        rhs[column] = cosines[column] * rhs[column]
        upper.append(entries[: column + 1])
    coeffs = [None] * M
    for row in reversed(range(M)):
        value = rhs[row]
        for later in range(row + 1, M):
            value = value - upper[later][row] * coeffs[later]
        coeffs[row] = value / upper[row][row]
    return coeffs, jnp.abs(rhs[M])


def finish_kernel(sums_ref, x_ref, r_ref, w1_ref, w2_ref, out_hbm, est_ref, out_ref, sem):
    parts = [(sums_ref[at] * SMALL, jnp.zeros((1, 128), F32)) for at in range(sums_ref.shape[0])]
    while len(parts) > 1:
        joined = []
        for at in range(0, len(parts) - 1, 2):
            s, e = two_sum(parts[at][0], parts[at + 1][0])
            joined.append((s, parts[at][1] + parts[at + 1][1] + e))
        parts = joined + parts[len(joined) * 2 :]
    high, low = parts[0]
    lane = lax.broadcasted_iota(jnp.int32, (1, 128), 1)
    pick = lambda row, at: jnp.sum(jnp.where(lane == at, row, 0.0), axis=1, keepdims=True)
    spread = lambda v: jnp.broadcast_to(v, (8, 128))
    m = [
        two_sum(spread(pick(high, at)), spread(pick(low, at) + pick(high, at + 8) + pick(low, at + 8)))
        for at in range(2 * M + 1)
    ]
    older, now = [None] * len(m), m
    ratio = m[1][0] / m[0][0]
    alphas, betas = [ratio], []
    previous = ratio
    for step in range(1, M + 1):
        new = [None] * len(m)
        for at in range(step, len(m) - step):
            value = minus_product(now[at + 1], alphas[step - 1], now[at])
            if step > 1:
                value = minus_product(value, betas[step - 2], older[at])
            new[at] = value
        betas.append(new[step][0] / now[step - 1][0])
        if step < M:
            ratio = new[step + 1][0] / new[step][0]
            alphas.append(ratio - previous)
            previous = ratio
        older, now = now, new
    offs = [jnp.sqrt(b) for b in betas]
    (y0, y1, y2), estimate = least_squares(alphas, offs)
    estimate = estimate * jnp.sqrt(m[0][0]) * (SMALL**-0.5)
    e1 = y1 / offs[0]
    e2 = y2 / (offs[0] * offs[1])
    c0 = (y0 - e1 * alphas[0] + e2 * (alphas[0] * alphas[1] - betas[0])) * (1.0 / SCALE)
    c1 = (e1 - e2 * (alphas[0] + alphas[1])) * (1.0 / SCALE)
    c2 = e2 * (1.0 / SCALE)
    est_ref[...] = estimate[0:1]
    planes, rows, lanes = x_ref.shape
    c0, c1, c2 = (jnp.broadcast_to(c[0:1, 0:1], (rows, lanes)) for c in (c0, c1, c2))
    step = 8

    def plane(x, carry):
        out_ref[x] = x_ref[x] + (c0 * r_ref[x] + c1 * w1_ref[x] + c2 * w2_ref[x])
        return carry

    copies = []
    for p in range(0, planes, step):
        lax.fori_loop(p, p + step, plane, 0)
        copy = pltpu.make_async_copy(out_ref.at[pl.ds(p, step)], out_hbm.at[pl.ds(p, step)], sem.at[p // step])
        copy.start()
        copies.append(copy)
    for copy in copies:
        copy.wait()


def local(sizes, right_side, start_guess, conductivity):
    shape = start_guess.shape
    planes, rows, lanes = shape
    devices = sizes[0] * sizes[1]
    block = vmem(shape)
    x_face, y_face = vmem((rows, lanes)), vmem((planes, lanes))
    faces = [x_face, x_face, y_face, y_face]
    pair = [vmem((2, rows, lanes))] * 2 + [vmem((2, planes, lanes))] * 2
    dma = pltpu.SemaphoreType.DMA
    work = 40 * planes * rows * lanes

    x0, kappa, *sends = call(
        functools.partial(faces_kernel, sizes), [block, block] + pair, 2, scratch=[dma((2,))], any_in=(0, 1), name="faces"
    )(start_guess, conductivity)
    halos = exchange(sends, sizes)
    r, cx, cy, cz, end = call(
        start_kernel, [block, vmem((planes + 1, rows, lanes)), block, block, block], 3, work,
        scratch=[block, dma((planes // 8,))], any_in=(2,), name="start",
    )(x0, kappa, right_side)
    r, *rest = call(
        functools.partial(start_fix_kernel, sizes), [block] + faces + faces, 9, aliases={0: 0}, name="start_fix"
    )(r, *sends, *halos)
    coeffs, sends = rest[:4], rest[4:]

    vectors, dots = [r], []
    for step in range(M):
        older = [vectors[-2]] if step else []
        last = step == M - 1
        count = 1 + len(older) + 2 * last
        halos = exchange(sends, sizes)
        w, sums = call(
            functools.partial(apply_kernel, len(older), last), [block, vmem((count, 8, 128))], 5 + len(older), work, name="apply"
        )(vectors[-1], cx, cy, cz, end, *older)
        dots.append(sums)
        if last:
            _, payload = call(
                functools.partial(last_fix_kernel, sizes), [block, vmem((devices, 1, 128))], 16, aliases={0: 0}, name="last_fix"
            )(w, *sends, *halos, *coeffs, *dots)
        else:
            w, *sends = call(
                functools.partial(fix_kernel, sizes), [block] + faces, 13, aliases={0: 0}, name="fix"
            )(w, *sends, *halos, *coeffs)
            vectors.append(w)
    sums = lax.all_to_all(payload, ("gx", "gy"), 0, 0, tiled=True)
    out, estimate = call(
        finish_kernel, [jax.ShapeDtypeStruct(shape, F32), jax.ShapeDtypeStruct((1, 128), F32)], 5,
        scratch=[block, dma((planes // 8,))], any_out=(0,), name="finish",
    )(sums, x0, *vectors)
    return out, estimate[0, 0]


def solution(mesh):
    sizes = (mesh.shape["gx"], mesh.shape["gy"])
    in_specs = (P("gx", "gy", None), P("gx", "gy", None), P("gx", "gy", None))
    out_specs = (P("gx", "gy", None), P())
    return jax.shard_map(
        functools.partial(local, sizes), mesh=mesh, in_specs=in_specs, out_specs=out_specs, check_vma=False
    )
```
